32 devices in a mesh: section: 8 (over z, y), fsdp: 4 (over x, core).
Axes of the slice: x: 2, y: 2, z: 4, core: 2. Of those that a mesh axis runs over, the one named last changes fastest.
Arguments:
- source_rows: bfloat16 [3072, 4096], P(('section', 'fsdp')), may hold values from -6 to 6
- target_rows: bfloat16 [1024, 4096], P('section'), may hold values from -6 to 6
- attn_weights: bfloat16 [8, 4, 4096, 3072], P('section', None, None, 'fsdp'), may hold values from -3.76875 to 3.76875
- gains: float32 [8, 4096], P('section'), may hold values from 0.25 to 1.75
- lengths: int32 [8], P('section'), may hold values from 192 to 384
Outputs:
- source_next: bfloat16 [3072, 4096], P(('section', 'fsdp'))
- target_next: bfloat16 [1024, 4096], P('section')
The draws below stay inside these ranges and needn't reach their ends.
Inputs may be any that keep to these rules, and one draw needn't show every extreme that they name: Keys at positions lengths[s] and beyond are padding.
All inputs are finite; a program needn't handle non-finite values.
Results may differ from the reference program's by a relative error of at most 0.015.
The reference program's roundings to bfloat16 on the way count: a program that leaves them out, or rounds other values in their place, can miss the bound.
Values may be sent and summed in bfloat16 or wider, within the bound.
No kernel may reach another device: no remote copies, remote signals or barrier semaphores. Data moves between devices by JAX's collectives and lax.ppermute only.
A program may use at most 128 MiB of HBM per device.

```python
import math
import jax
import jax.numpy as jnp
from jax import lax

D = 4096
HEAD_DIM = 64
IN_LEN = 384
OUT_LEN = 128
INNER = 3072
SOURCE_TOTAL = 3072
TARGET_TOTAL = 1024
N_SECTION = 8
N_FSDP = 4


def draw_attn_weights(key, part):
    shape_all = (N_SECTION, 4, D, INNER)
    drawn = jnp.clip(jax.random.normal(key, shape_all, jnp.float32), -6.0, 6.0) / math.sqrt(D)
    return drawn.astype(jnp.bfloat16)


def touch_ends(array, stream_key, least, high):
    longest = array.shape.index(max(array.shape))
    spots = []
    for shift in (0, 1):
        where = [jax.random.randint(jax.random.fold_in(stream_key, axis), (), 0, length) for axis, length in enumerate(array.shape)]
        where[longest] = (where[longest] + shift) % array.shape[longest]
        spots.append(tuple(where))
    return array.at[spots[0]].set(least).at[spots[1]].set(high)


def block_levels(rng, extent, shards, smallest, high):
    gain, own = 1.0, jax.random.fold_in(rng, 6)
    for position, parts in shards:
        draws = jnp.exp(jax.random.uniform(jax.random.fold_in(own, position), (parts,), jnp.float32, smallest / len(shards), high / len(shards)))
        gain = gain * jnp.repeat(draws, extent[position] // parts).reshape([-1 if axis == position else 1 for axis in range(len(extent))])
    return gain


def centred(stream_key, shape, deviation, limit, split=(), kind=jnp.bfloat16):
    result = deviation * jax.random.normal(stream_key, shape, jnp.float32)
    if split:
        result = result * block_levels(stream_key, shape, split, -0.22, 0.18)
    return jnp.clip(result, -limit, limit).astype(kind)


def setup_inputs(seed: int = 0) -> dict:
    keys = jax.random.split(jax.random.key(seed), 6)
    source_rows = centred(keys[0], (SOURCE_TOTAL, D), 1.0, 6.0, ((0, 32),))
    target_rows = centred(keys[1], (TARGET_TOTAL, D), 1.0, 6.0, ((0, 8),))
    attn_weights = draw_attn_weights(jax.random.fold_in(keys[5], 71), 0)
    gains = jnp.clip(1.0 + 0.15 * jax.random.normal(keys[3], (N_SECTION, D), jnp.float32), 0.25, 1.75)
    lengths = touch_ends(jax.random.randint(keys[4], (N_SECTION,), IN_LEN // 2, IN_LEN + 1), jax.random.fold_in(keys[4], 1), IN_LEN // 2, IN_LEN).astype(jnp.int32)
    return dict(source_rows=source_rows, target_rows=target_rows, attn_weights=attn_weights, gains=gains, lengths=lengths)


def rms_norm(block_rows, gain_row):
    widened = block_rows.astype(jnp.float32)
    inverse_rms = lax.rsqrt(lax.optimization_barrier(jnp.mean(widened * widened, axis=-1, keepdims=True)) + 1e-06)
    return (widened * inverse_rms * gain_row).astype(jnp.bfloat16)

def project(block_rows, weight):
    return jnp.dot(block_rows, weight, preferred_element_type=jnp.float32).astype(jnp.bfloat16)

def attend(queries, key_rows, values, length):
    query_count = queries.shape[0]
    key_count = key_rows.shape[0]
    head_count = queries.shape[1] // HEAD_DIM
    query_heads = queries.reshape(query_count, head_count, HEAD_DIM).astype(jnp.float32)
    key_heads = key_rows.reshape(key_count, head_count, HEAD_DIM).astype(jnp.float32)
    value_heads = values.reshape(key_count, head_count, HEAD_DIM).astype(jnp.float32)
    scores = jnp.einsum('qhc,khc->hqk', query_heads, key_heads) * 0.125
    key_valid = jnp.arange(key_count, dtype=jnp.int32) < length
    scores = jnp.where(key_valid[None, None, :], scores, -1000000000.0)
    row_max = lax.optimization_barrier(jnp.max(scores, axis=-1, keepdims=True))
    expo = jnp.exp(scores - row_max)
    soft = (expo / lax.optimization_barrier(jnp.sum(expo, axis=-1, keepdims=True))).astype(jnp.bfloat16)
    context = jnp.einsum('hqk,khc->qhc', soft.astype(jnp.float32), value_heads)
    return context.reshape(query_count, head_count * HEAD_DIM).astype(jnp.bfloat16)

def out_terms(context, out_weight):
    row_count = context.shape[0]
    context_groups = context.reshape(row_count, N_FSDP, -1).astype(jnp.float32)
    weight_groups = out_weight.reshape(out_weight.shape[0], N_FSDP, -1).astype(jnp.float32)
    group_terms = jnp.einsum('rgc,dgc->grd', context_groups, weight_groups)
    rounded = lax.optimization_barrier(group_terms.astype(jnp.bfloat16))
    return lax.optimization_barrier(jnp.sum(rounded.astype(jnp.float32), axis=0))

def reference(source_rows, target_rows, attn_weights, gains, lengths):
    half_sections = N_SECTION // 2
    source_blocks = source_rows.reshape(N_SECTION, IN_LEN, D)
    target_blocks = target_rows.reshape(N_SECTION, OUT_LEN, D)
    source_out = []
    target_out = []
    for section_index in range(N_SECTION):
        weights = attn_weights[section_index]
        gain_row = gains[section_index]
        length = lengths[section_index]
        source_block = source_blocks[section_index]
        target_block = target_blocks[section_index]
        if section_index < half_sections:
            normed = rms_norm(source_block, gain_row)
            context = attend(project(normed, weights[0]), project(normed, weights[1]), project(normed, weights[2]), length)
            source_block = (source_block.astype(jnp.float32) + out_terms(context, weights[3])).astype(jnp.bfloat16)
        else:
            normed = rms_norm(target_block, gain_row)
            context = attend(project(normed, weights[0]), project(source_block, weights[1]), project(source_block, weights[2]), length)
            target_block = (target_block.astype(jnp.float32) + out_terms(context, weights[3])).astype(jnp.bfloat16)
        source_out.append(source_block)
        target_out.append(target_block)
    source_next = jnp.roll(jnp.stack(source_out), 1, axis=0).reshape(N_SECTION * IN_LEN, D)
    target_next = jnp.roll(jnp.stack(target_out), 1, axis=0).reshape(N_SECTION * OUT_LEN, D)
    return (source_next, target_next)
```

```python
import functools
import jax
import jax.numpy as jnp
from jax import lax
from jax.experimental import pallas as pl
from jax.experimental.pallas import tpu as pltpu
from jax.sharding import PartitionSpec as P

HEAD_DIM = 64
LOG2E = 1.4426950408889634


def shifted(value, axis, steps):
    count = lax.axis_size(axis)
    pairs = [(source, (source + steps) % count) for source in range(count)]
    return lax.ppermute(value, axis, pairs)


def rms_norm(block_rows, gain_row):
    widened = block_rows.astype(jnp.float32)
    inverse_rms = lax.rsqrt(jnp.mean(widened * widened, axis=-1, keepdims=True) + 1e-06)
    return (widened * inverse_rms * gain_row).astype(jnp.bfloat16)


def project(block_rows, weight):
    return jnp.dot(block_rows, weight, preferred_element_type=jnp.float32).astype(jnp.bfloat16)


def attend(queries, key_rows, values, length):
    query_count = queries.shape[0]
    key_count = key_rows.shape[0]
    head_count = queries.shape[1] // HEAD_DIM
    query_heads = queries.reshape(query_count, head_count, HEAD_DIM)
    key_heads = key_rows.reshape(key_count, head_count, HEAD_DIM)
    value_heads = values.reshape(key_count, head_count, HEAD_DIM)
    scores = (
        jnp.einsum("qhc,khc->hqk", query_heads, key_heads, preferred_element_type=jnp.float32)
        * 0.125
    )
    key_valid = jnp.arange(key_count, dtype=jnp.int32) < length
    scores = jnp.where(key_valid[None, None, :], scores, -1000000000.0)
    row_max = jnp.max(scores, axis=-1, keepdims=True)
    expo = jnp.exp(scores - row_max)
    soft = (expo / jnp.sum(expo, axis=-1, keepdims=True)).astype(jnp.bfloat16)
    context = jnp.einsum("hqk,khc->qhc", soft, value_heads, preferred_element_type=jnp.float32)
    return context.reshape(query_count, head_count * HEAD_DIM).astype(jnp.bfloat16)


def out_partial(context, out_weight):
    return lax.dot_general(
        context, out_weight, (((1,), (1,)), ((), ())), preferred_element_type=jnp.float32
    )


def local_general(source_rows, target_rows, attn_weights, gains, lengths):
    section_index = lax.axis_index("section")
    encoder_section = section_index < lax.axis_size("section") // 2
    weights = attn_weights[0]
    gain_row = gains[0]
    length = lengths[0]
    source_whole = lax.all_gather(source_rows, "fsdp", axis=0, tiled=True)

    def encoder_work(whole_rows, target_block):
        normed = rms_norm(whole_rows, gain_row)
        context = attend(
            project(normed, weights[0]),
            project(normed, weights[1]),
            project(normed, weights[2]),
            length,
        )
        return (out_partial(context, weights[3]), jnp.zeros(target_block.shape, jnp.float32))

    def decoder_work(whole_rows, target_block):
        normed = rms_norm(target_block, gain_row)
        context = attend(
            project(normed, weights[0]),
            project(whole_rows, weights[1]),
            project(whole_rows, weights[2]),
            length,
        )
        return (jnp.zeros(whole_rows.shape, jnp.float32), out_partial(context, weights[3]))

    source_terms, target_terms = lax.cond(
        encoder_section, encoder_work, decoder_work, source_whole, target_rows
    )
    source_sum = lax.psum_scatter(
        source_terms.astype(jnp.bfloat16), "fsdp", scatter_dimension=0, tiled=True
    ).astype(jnp.float32)
    source_new = (source_rows.astype(jnp.float32) + source_sum).astype(jnp.bfloat16)
    target_sum = lax.psum(target_terms.astype(jnp.bfloat16), "fsdp").astype(jnp.float32)
    target_new = (target_rows.astype(jnp.float32) + target_sum).astype(jnp.bfloat16)
    source_next, target_next = shifted((source_new, target_new), "section", 1)
    return (source_next, target_next)


def norm_kernel(ids, x_ref, gain_ref, o_ref):
    @pl.when(ids[0] == 1)
    def _():
        o_ref[...] = rms_norm(x_ref[...], gain_ref[...])

    @pl.when(ids[0] == 0)
    def _():
        o_ref[...] = x_ref[...]


def norm_rows(ids, rows, gains):
    count, width = rows.shape
    return pl.pallas_call(
        norm_kernel,
        grid_spec=pltpu.PrefetchScalarGridSpec(
            num_scalar_prefetch=1,
            grid=(1,),
            in_specs=[
                pl.BlockSpec((count, width), lambda i, s: (0, 0)),
                pl.BlockSpec((1, width), lambda i, s: (0, 0)),
            ],
            out_specs=pl.BlockSpec((count, width), lambda i, s: (0, 0)),
        ),
        out_shape=jax.ShapeDtypeStruct(rows.shape, jnp.bfloat16),
        cost_estimate=pl.CostEstimate(
            flops=count * width * 200, bytes_accessed=count * width * 4, transcendentals=0
        ),
        name="norm_rows",
    )(ids, rows, gains)


def qkv_kernel(n_pieces, part, n_query, slot_index, ids, *refs):
    pieces = refs[:n_pieces]
    sibling_pieces = refs[n_pieces : 2 * n_pieces]
    y_ref, gain_ref, w_ref = refs[2 * n_pieces : 2 * n_pieces + 3]
    o_ref, x_all, y_all = refs[-3:]
    step = pl.program_id(0)
    encoder, core = ids[0], ids[2]
    rows = x_all.shape[0] // 2
    piece = rows // n_pieces

    @pl.when(step == 0)
    def _():
        for index in range(n_pieces):
            mine = pl.multiple_of(core * rows + index * piece, piece)
            other = pl.multiple_of((1 - core) * rows + index * piece, piece)
            x_all[pl.ds(mine, piece), :] = pieces[index][...]
            x_all[pl.ds(other, piece), :] = sibling_pieces[index][...]

        @pl.when(encoder == 0)
        def _():
            y_all[...] = rms_norm(y_ref[...], gain_ref[...])

    from_target = jnp.logical_and(encoder == 0, step < n_query)

    @pl.when(jnp.logical_not(from_target))
    def _():
        o_ref[...] = jnp.dot(
            x_all[...], w_ref[...], preferred_element_type=jnp.float32
        ).astype(jnp.bfloat16)

    @pl.when(from_target)
    def _():
        queries = jnp.dot(
            y_all[...], w_ref[...], preferred_element_type=jnp.float32
        ).astype(jnp.bfloat16)
        half = queries.shape[0] // 2
        o_ref[...] = jnp.zeros_like(o_ref)
        o_ref[0:half, :] = queries[:half]
        o_ref[rows : rows + half, :] = queries[half:]


def qkv_rows(ids, pieces, sibling_pieces, target_rows, gains, attn_weights, slot_index, into):
    n_pieces = len(pieces)
    rows = sum(p.shape[0] for p in pieces)
    width = pieces[0].shape[1]
    inner = attn_weights.shape[3]
    tile = 256
    per = inner // tile
    part = target_rows.shape[0] // 2
    in_specs = [pl.BlockSpec(p.shape, lambda i, s: (0, 0)) for p in pieces + sibling_pieces]
    in_specs += [
        pl.BlockSpec((part, width), lambda i, s: (s[slot_index], 0)),
        pl.BlockSpec((1, width), lambda i, s: (0, 0)),
        pl.BlockSpec((None, None, width, tile), lambda i, s: (0, i // per, 0, i % per)),
    ]
    operands = [ids, *pieces, *sibling_pieces, target_rows, gains, attn_weights]
    aliases = {}
    if into is not None:
        in_specs.append(pl.BlockSpec(memory_space=pl.ANY))
        aliases = {len(operands): 0}
        operands.append(into)
    return pl.pallas_call(
        functools.partial(qkv_kernel, n_pieces, part, per, slot_index),
        grid_spec=pltpu.PrefetchScalarGridSpec(
            num_scalar_prefetch=1,
            grid=(3 * per,),
            in_specs=in_specs,
            out_specs=pl.BlockSpec((2 * rows, tile), lambda i, s: (s[slot_index], i)),
            scratch_shapes=[
                pltpu.VMEM((2 * rows, width), jnp.bfloat16),
                pltpu.VMEM((part, width), jnp.bfloat16),
            ],
        ),
        out_shape=jax.ShapeDtypeStruct((4 * rows, 3 * inner), jnp.bfloat16),
        input_output_aliases=aliases,
        cost_estimate=pl.CostEstimate(
            flops=2 * 2 * rows * width * 3 * inner,
            bytes_accessed=2 * width * 3 * inner,
            transcendentals=0,
        ),
        name="qkv_rows",
    )(*operands)


def attend_kernel(ids, q0, q1, q2, q3, k_ref, v_ref, w_ref, keep_ref, send_ref, ctx):
    @pl.when(pl.program_id(0) == 0)
    def _():
        length = ids[4]
        queries = jnp.concatenate([q[...] for q in (q0, q1, q2, q3)], axis=0)
        rows, inner = queries.shape
        count = k_ref.shape[0]
        valid = lax.broadcasted_iota(jnp.int32, (rows, count), 1) < length
        low = lax.broadcasted_iota(jnp.int32, (rows, 2 * HEAD_DIM), 1) < HEAD_DIM
        for pair in range(inner // (2 * HEAD_DIM)):
            lanes = slice(pair * 2 * HEAD_DIM, (pair + 1) * 2 * HEAD_DIM)
            q_pair = queries[:, lanes]
            k_pair = k_ref[:, lanes]
            v_pair = v_ref[:, lanes]
            parts = []
            for head in range(2):
                mask = low if head == 0 else jnp.logical_not(low)
                q_head = jnp.where(mask, q_pair, jnp.zeros_like(q_pair))
                scores = lax.dot_general(
                    q_head, k_pair, (((1,), (1,)), ((), ())), preferred_element_type=jnp.float32
                )
                scores = jnp.where(valid, scores, -8000000000.0)
                row_max = jnp.max(scores, axis=-1, keepdims=True)
                expo = jnp.exp2((scores - row_max) * (0.125 * LOG2E))
                total = jnp.sum(expo, axis=-1, keepdims=True)
                soft = (expo * (1.0 / total)).astype(jnp.bfloat16)
                parts.append(jnp.dot(soft, v_pair, preferred_element_type=jnp.float32))
            ctx[:, lanes] = jnp.where(low, parts[0], parts[1]).astype(jnp.bfloat16)

    terms = out_partial(ctx[...], w_ref[...]).astype(jnp.bfloat16)
    half = terms.shape[0] // 2
    keep_ref[...] = terms[:half]
    send_ref[...] = terms[half:]


def attend_chunk(ids, qkv, attn_weights, chunk, chunks):
    total, inner = qkv.shape[0], attn_weights.shape[3]
    width = attn_weights.shape[2]
    rows = total // (4 * chunks)
    tile = 512
    query = qkv.reshape(4, chunks, rows, qkv.shape[1])

    def query_spec(order):
        return pl.BlockSpec((None, None, rows, inner), lambda i, s: (s[order], chunk, 0, 0))

    half = jax.ShapeDtypeStruct((2 * rows, width), jnp.bfloat16)
    return pl.pallas_call(
        attend_kernel,
        grid_spec=pltpu.PrefetchScalarGridSpec(
            num_scalar_prefetch=1,
            grid=(width // tile,),
            in_specs=[
                query_spec(5),
                query_spec(6),
                query_spec(7),
                query_spec(8),
                pl.BlockSpec((total, inner), lambda i, s: (0, 1)),
                pl.BlockSpec((total, inner), lambda i, s: (0, 2)),
                pl.BlockSpec((None, None, tile, inner), lambda i, s: (0, 3, i, 0)),
            ],
            out_specs=[
                pl.BlockSpec((2 * rows, tile), lambda i, s: (0, i)),
                pl.BlockSpec((2 * rows, tile), lambda i, s: (0, i)),
            ],
            scratch_shapes=[pltpu.VMEM((4 * rows, inner), jnp.bfloat16)],
        ),
        out_shape=[half, half],
        cost_estimate=pl.CostEstimate(
            flops=6 * 2 * 4 * rows * width * inner,
            bytes_accessed=2 * width * inner,
            transcendentals=0,
        ),
        name="attend_chunk",
    )(ids, query, query, query, query, qkv, qkv, attn_weights)


def local_pairs(chunks, source_rows, target_rows, attn_weights, gains, lengths):
    f32, bf16 = jnp.float32, jnp.bfloat16
    n_section = lax.axis_size("section")
    n_encoder = n_section // 2
    section = lax.axis_index("section")
    here = lax.axis_index("fsdp")
    chip, core = here // 2, here % 2
    is_encoder = section < n_encoder
    ids = jnp.stack(
        [
            is_encoder.astype(jnp.int32),
            chip,
            core,
            1 - chip,
            lengths[0],
            here,
            here ^ 2,
            here ^ 1,
            here ^ 3,
        ]
    ).astype(jnp.int32)
    piece = source_rows.shape[0] // chunks

    def to_sibling(value):
        return lax.ppermute(value, "fsdp", [(0, 1), (1, 0), (2, 3), (3, 2)])

    def across(value):
        return lax.ppermute(value, "fsdp", [(0, 2), (2, 0), (1, 3), (3, 1)])

    def onward(value, first, last):
        pairs = [(s, (s + 1) % n_section) for s in range(first, last)]
        return lax.ppermute(value, "section", pairs)

    normed = norm_rows(ids, source_rows, gains)
    remote = [across(normed[i * piece : (i + 1) * piece]) for i in range(chunks)]
    near = to_sibling(normed)
    early_source = onward(source_rows, n_encoder, n_section)
    early_target = onward(target_rows, 0, n_encoder)
    qkv = qkv_rows(ids, [normed], [near], target_rows, gains, attn_weights, 1, None)
    remote_near = [to_sibling(r) for r in remote]
    qkv = qkv_rows(ids, remote, remote_near, target_rows, gains, attn_weights, 3, qkv)

    target_piece = lax.dynamic_slice_in_dim(target_rows, here * piece, piece, 0)
    moved = []
    for chunk in range(chunks):
        residual = source_rows[chunk * piece : (chunk + 1) * piece]
        if chunk == 0:
            residual = jnp.where(is_encoder, residual, target_piece)
        keep, send = attend_chunk(ids, qkv, attn_weights, chunk, chunks)
        taken = to_sibling(send)
        for_other = (keep[piece:].astype(f32) + taken[piece:].astype(f32)).astype(bf16)
        crossed = across(for_other)
        total = keep[:piece].astype(f32) + taken[:piece].astype(f32) + crossed.astype(f32)
        new = (residual.astype(f32) + total).astype(bf16)
        moved.append(onward(new, 0, n_section if chunk == 0 else n_encoder))

    first = moved[0]
    first_across = across(first)
    both_near = to_sibling(jnp.stack([first, first_across]))
    by_offset = jnp.stack([first, both_near[0], first_across, both_near[1]])
    by_core = jnp.where(core == 1, by_offset[jnp.array([1, 0, 3, 2])], by_offset)
    ordered = jnp.where(chip == 1, jnp.roll(by_core, 2, axis=0), by_core)
    came_from_encoder = jnp.logical_and(section >= 1, section <= n_encoder)
    source_next = jnp.where(came_from_encoder, jnp.concatenate(moved, axis=0), early_source)
    target_next = jnp.where(
        came_from_encoder, early_target, ordered.reshape(target_rows.shape)
    )
    return (source_next, target_next)


def solution(mesh):
    in_specs = (
        P(("section", "fsdp"), None),
        P("section", None),
        P("section", None, None, "fsdp"),
        P("section", None),
        P("section"),
    )
    out_specs = (P(("section", "fsdp"), None), P("section", None))

    def run(source_rows, target_rows, attn_weights, gains, lengths):
        n_section, n_fsdp = mesh.shape["section"], mesh.shape["fsdp"]
        own = source_rows.shape[0] // (n_section * n_fsdp)
        part = target_rows.shape[0] // (n_section * n_fsdp)
        paired = (
            n_fsdp == 4
            and part * n_section * n_fsdp == target_rows.shape[0]
            and part % 16 == 0
            and own % part == 0
            and attn_weights.shape[3] // n_fsdp % 256 == 0
            and attn_weights.shape[2] % 512 == 0
        )
        body = functools.partial(local_pairs, own // part) if paired else local_general
        return jax.shard_map(
            body, mesh=mesh, in_specs=in_specs, out_specs=out_specs, check_vma=False
        )(source_rows, target_rows, attn_weights, gains, lengths)

    return run
```

```python
import functools
import jax
import jax.numpy as jnp
from jax import lax
from jax.experimental import pallas as pl
from jax.experimental.pallas import tpu as pltpu
from jax.sharding import PartitionSpec as P

HEAD_DIM = 64
LOG2E = 1.4426950408889634


def shifted(value, axis, steps):
    count = lax.axis_size(axis)
    pairs = [(source, (source + steps) % count) for source in range(count)]
    return lax.ppermute(value, axis, pairs)


def rms_norm(block_rows, gain_row):
    widened = block_rows.astype(jnp.float32)
    inverse_rms = lax.rsqrt(jnp.mean(widened * widened, axis=-1, keepdims=True) + 1e-06)
    return (widened * inverse_rms * gain_row).astype(jnp.bfloat16)


def project(block_rows, weight):
    return jnp.dot(block_rows, weight, preferred_element_type=jnp.float32).astype(jnp.bfloat16)


def attend(queries, key_rows, values, length):
    query_count = queries.shape[0]
    key_count = key_rows.shape[0]
    head_count = queries.shape[1] // HEAD_DIM
    query_heads = queries.reshape(query_count, head_count, HEAD_DIM)
    key_heads = key_rows.reshape(key_count, head_count, HEAD_DIM)
    value_heads = values.reshape(key_count, head_count, HEAD_DIM)
    scores = (
        jnp.einsum("qhc,khc->hqk", query_heads, key_heads, preferred_element_type=jnp.float32)
        * 0.125
    )
    key_valid = jnp.arange(key_count, dtype=jnp.int32) < length
    scores = jnp.where(key_valid[None, None, :], scores, -1000000000.0)
    row_max = jnp.max(scores, axis=-1, keepdims=True)
    expo = jnp.exp(scores - row_max)
    soft = (expo / jnp.sum(expo, axis=-1, keepdims=True)).astype(jnp.bfloat16)
    context = jnp.einsum("hqk,khc->qhc", soft, value_heads, preferred_element_type=jnp.float32)
    return context.reshape(query_count, head_count * HEAD_DIM).astype(jnp.bfloat16)


def out_partial(context, out_weight):
    return lax.dot_general(
        context, out_weight, (((1,), (1,)), ((), ())), preferred_element_type=jnp.float32
    )


def local_general(source_rows, target_rows, attn_weights, gains, lengths):
    section_index = lax.axis_index("section")
    encoder_section = section_index < lax.axis_size("section") // 2
    weights = attn_weights[0]
    gain_row = gains[0]
    length = lengths[0]
    source_whole = lax.all_gather(source_rows, "fsdp", axis=0, tiled=True)

    def encoder_work(whole_rows, target_block):
        normed = rms_norm(whole_rows, gain_row)
        context = attend(
            project(normed, weights[0]),
            project(normed, weights[1]),
            project(normed, weights[2]),
            length,
        )
        return (out_partial(context, weights[3]), jnp.zeros(target_block.shape, jnp.float32))

    def decoder_work(whole_rows, target_block):
        normed = rms_norm(target_block, gain_row)
        context = attend(
            project(normed, weights[0]),
            project(whole_rows, weights[1]),
            project(whole_rows, weights[2]),
            length,
        )
        return (jnp.zeros(whole_rows.shape, jnp.float32), out_partial(context, weights[3]))

    source_terms, target_terms = lax.cond(
        encoder_section, encoder_work, decoder_work, source_whole, target_rows
    )
    source_sum = lax.psum_scatter(
        source_terms.astype(jnp.bfloat16), "fsdp", scatter_dimension=0, tiled=True
    ).astype(jnp.float32)
    source_new = (source_rows.astype(jnp.float32) + source_sum).astype(jnp.bfloat16)
    target_sum = lax.psum(target_terms.astype(jnp.bfloat16), "fsdp").astype(jnp.float32)
    target_new = (target_rows.astype(jnp.float32) + target_sum).astype(jnp.bfloat16)
    source_next, target_next = shifted((source_new, target_new), "section", 1)
    return (source_next, target_next)


PARAMS = pltpu.CompilerParams(vmem_limit_bytes=24 * 1024 * 1024)
PARTS = 4
WEIGHT_PARAMS = pltpu.CompilerParams(vmem_limit_bytes=42 * 1024 * 1024)


def norm_kernel(ids, x_ref, gain_ref, *outs):
    piece = outs[1].shape[0]

    def put(value):
        outs[0][...] = value
        for index, out in enumerate(outs[1:]):
            out[...] = value[index * piece : (index + 1) * piece]

    @pl.when(ids[0] == 1)
    def _():
        put(rms_norm(x_ref[...], gain_ref[...]))

    @pl.when(ids[0] == 0)
    def _():
        put(x_ref[...])


def norm_rows(ids, rows, gains, chunks):
    count, width = rows.shape
    shapes = [(count, width)] + [(count // chunks, width)] * chunks
    return pl.pallas_call(
        norm_kernel,
        grid_spec=pltpu.PrefetchScalarGridSpec(
            num_scalar_prefetch=1,
            grid=(1,),
            in_specs=[
                pl.BlockSpec((count, width), lambda i, s: (0, 0)),
                pl.BlockSpec((1, width), lambda i, s: (0, 0)),
            ],
            out_specs=[pl.BlockSpec(shape, lambda i, s: (0, 0)) for shape in shapes],
        ),
        out_shape=[jax.ShapeDtypeStruct(shape, jnp.bfloat16) for shape in shapes],
        compiler_params=PARAMS,
        cost_estimate=pl.CostEstimate(
            flops=count * width * 200, bytes_accessed=count * width * 4, transcendentals=0
        ),
        name="norm_rows",
    )(ids, rows, gains)


def qkv_kernel(n_pieces, n_query, ids, *refs):
    pieces = refs[:n_pieces]
    sibling_pieces = refs[n_pieces : 2 * n_pieces]
    y_ref, gain_ref, w_ref = refs[2 * n_pieces : 2 * n_pieces + 3]
    o_ref, x_all, y_all = refs[-3:]
    step = pl.program_id(0)
    encoder, core = ids[0], ids[2]
    rows = x_all.shape[0] // 2
    piece = rows // n_pieces

    @pl.when(step == 0)
    def _():
        for index in range(n_pieces):
            mine = pl.multiple_of(core * rows + index * piece, piece)
            other = pl.multiple_of((1 - core) * rows + index * piece, piece)
            x_all[pl.ds(mine, piece), :] = pieces[index][...]
            x_all[pl.ds(other, piece), :] = sibling_pieces[index][...]

        @pl.when(encoder == 0)
        def _():
            y_all[...] = rms_norm(y_ref[...], gain_ref[...])

    from_target = jnp.logical_and(encoder == 0, step < n_query)

    @pl.when(jnp.logical_not(from_target))
    def _():
        o_ref[...] = jnp.dot(
            x_all[...], w_ref[...], preferred_element_type=jnp.float32
        ).astype(jnp.bfloat16)

    @pl.when(from_target)
    def _():
        queries = jnp.dot(
            y_all[...], w_ref[...], preferred_element_type=jnp.float32
        ).astype(jnp.bfloat16)
        half = queries.shape[0] // 2
        o_ref[...] = jnp.zeros_like(o_ref)
        o_ref[0:half, :] = queries[:half]
        o_ref[rows : rows + half, :] = queries[half:]


def qkv_rows(ids, pieces, sibling_pieces, target_rows, gains, attn_weights, slot_index, into):
    n_pieces = len(pieces)
    rows = sum(p.shape[0] for p in pieces)
    width = pieces[0].shape[1]
    inner = attn_weights.shape[3]
    tile = 256
    per = inner // tile
    part = target_rows.shape[0] // 2
    in_specs = [pl.BlockSpec(p.shape, lambda i, s: (0, 0)) for p in pieces + sibling_pieces]
    in_specs += [
        pl.BlockSpec((part, width), lambda i, s: (s[slot_index], 0)),
        pl.BlockSpec((1, width), lambda i, s: (0, 0)),
        pl.BlockSpec((None, None, width, tile), lambda i, s: (0, i // per, 0, i % per)),
    ]
    operands = [ids, *pieces, *sibling_pieces, target_rows, gains, attn_weights]
    aliases = {}
    if into is not None:
        in_specs.append(pl.BlockSpec(memory_space=pl.ANY))
        aliases = {len(operands): 0}
        operands.append(into)
    return pl.pallas_call(
        functools.partial(qkv_kernel, n_pieces, per),
        grid_spec=pltpu.PrefetchScalarGridSpec(
            num_scalar_prefetch=1,
            grid=(3 * per,),
            in_specs=in_specs,
            out_specs=pl.BlockSpec((2 * rows, tile), lambda i, s: (s[slot_index], i)),
            scratch_shapes=[
                pltpu.VMEM((2 * rows, width), jnp.bfloat16),
                pltpu.VMEM((part, width), jnp.bfloat16),
            ],
        ),
        out_shape=jax.ShapeDtypeStruct((4 * rows, 3 * inner), jnp.bfloat16),
        input_output_aliases=aliases,
        cost_estimate=pl.CostEstimate(
            flops=2 * 2 * rows * width * 3 * inner,
            bytes_accessed=2 * width * 3 * inner,
            transcendentals=0,
        ),
        compiler_params=WEIGHT_PARAMS,
        name="qkv_rows",
    )(*operands)


def attend_kernel(ids, q_ref, k_ref, v_ref, ctx):
    length = ids[4]
    rows, inner = q_ref.shape
    count = k_ref.shape[0]
    valid = lax.broadcasted_iota(jnp.int32, (rows, count), 1) < length
    low = lax.broadcasted_iota(jnp.int32, (rows, 2 * HEAD_DIM), 1) < HEAD_DIM
    for pair in range(inner // (2 * HEAD_DIM)):
        lanes = slice(pair * 2 * HEAD_DIM, (pair + 1) * 2 * HEAD_DIM)
        q_pair = q_ref[:, lanes]
        k_pair = k_ref[:, lanes]
        v_pair = v_ref[:, lanes]
        parts = []
        for head in range(2):
            mask = low if head == 0 else jnp.logical_not(low)
            q_head = jnp.where(mask, q_pair, jnp.zeros_like(q_pair))
            scores = lax.dot_general(
                q_head, k_pair, (((1,), (1,)), ((), ())), preferred_element_type=jnp.float32
            )
            scores = jnp.where(valid, scores, -8000000000.0)
            row_max = jnp.max(scores, axis=-1, keepdims=True)
            expo = jnp.exp2((scores - row_max) * (0.125 * LOG2E))
            total = jnp.sum(expo, axis=-1, keepdims=True)
            soft = (expo * (1.0 / total)).astype(jnp.bfloat16)
            parts.append(jnp.dot(soft, v_pair, preferred_element_type=jnp.float32))
        ctx[:, lanes] = jnp.where(low, parts[0], parts[1]).astype(jnp.bfloat16)


def attend_rows(ids, qkv, inner):
    total = qkv.shape[0]
    return pl.pallas_call(
        attend_kernel,
        grid_spec=pltpu.PrefetchScalarGridSpec(
            num_scalar_prefetch=1,
            grid=(1,),
            in_specs=[
                pl.BlockSpec((total, inner), lambda i, s: (0, 0)),
                pl.BlockSpec((total, inner), lambda i, s: (0, 1)),
                pl.BlockSpec((total, inner), lambda i, s: (0, 2)),
            ],
            out_specs=pl.BlockSpec((total, inner), lambda i, s: (0, 0)),
        ),
        out_shape=jax.ShapeDtypeStruct((total, inner), jnp.bfloat16),
        compiler_params=PARAMS,
        cost_estimate=pl.CostEstimate(
            flops=40 * total * total * inner, bytes_accessed=8 * total * inner, transcendentals=0
        ),
        name="attend_rows",
    )(ids, qkv, qkv, qkv)


def out_kernel(ids, c0, c1, c2, c3, w_ref, keep_ref, send_ref):
    context = jnp.concatenate([c[...] for c in (c0, c1, c2, c3)], axis=0)
    terms = out_partial(context, w_ref[...]).astype(jnp.bfloat16)
    half = terms.shape[0] // 2
    keep_ref[...] = terms[:half]
    send_ref[...] = terms[half:]


def out_chunk(ids, context, attn_weights, chunk, parts):
    total, inner = context.shape
    span = attn_weights.shape[2] // parts
    tile = span // 2

    def rows_spec(slot):
        return pl.BlockSpec((total // 4, inner), lambda i, s: (s[slot], 0))

    half = jax.ShapeDtypeStruct((total // 2, span), jnp.bfloat16)
    return pl.pallas_call(
        out_kernel,
        grid_spec=pltpu.PrefetchScalarGridSpec(
            num_scalar_prefetch=1,
            grid=(2,),
            in_specs=[
                rows_spec(5),
                rows_spec(6),
                rows_spec(7),
                rows_spec(8),
                pl.BlockSpec((None, None, tile, inner), lambda i, s: (0, 3, 2 * chunk + i, 0)),
            ],
            out_specs=[pl.BlockSpec((total // 2, tile), lambda i, s: (0, i))] * 2,
        ),
        out_shape=[half, half],
        compiler_params=WEIGHT_PARAMS,
        cost_estimate=pl.CostEstimate(
            flops=2 * total * span * inner, bytes_accessed=2 * span * inner, transcendentals=0
        ),
        name="out_chunk",
    )(ids, context, context, context, context, attn_weights)


def small_call(kernel, ids, operands, blocks, out_shape):
    def spec(shape, index):
        row, column = index
        if row == "here":
            return pl.BlockSpec(shape, lambda i, s: (s[5], column))
        return pl.BlockSpec(shape, lambda i, s: (row, column))

    return pl.pallas_call(
        kernel,
        grid_spec=pltpu.PrefetchScalarGridSpec(
            num_scalar_prefetch=1,
            grid=(1,),
            in_specs=[spec(*b) for b in blocks],
            out_specs=pl.BlockSpec(out_shape, lambda i, s: (0, 0)),
        ),
        out_shape=jax.ShapeDtypeStruct(out_shape, jnp.bfloat16),
        compiler_params=PARAMS,
        cost_estimate=pl.CostEstimate(
            flops=out_shape[0] * out_shape[1] * 200,
            bytes_accessed=out_shape[0] * out_shape[1] * 8,
            transcendentals=0,
        ),
    )(ids, *operands)


def pair_kernel(ids, keep_ref, taken_ref, o_ref):
    o_ref[...] = (
        keep_ref[...].astype(jnp.float32) + taken_ref[...].astype(jnp.float32)
    ).astype(jnp.bfloat16)


def final_kernel(ids, keep_ref, taken_ref, crossed_ref, source_ref, target_ref, o_ref):
    f32 = jnp.float32
    total = keep_ref[...].astype(f32) + taken_ref[...].astype(f32) + crossed_ref[...].astype(f32)
    o_ref[...] = (source_ref[...].astype(f32) + total).astype(jnp.bfloat16)

    @pl.when(ids[0] == 0)
    def _():
        part = target_ref.shape[0]
        o_ref[0:part, :] = (target_ref[...].astype(f32) + total[:part]).astype(jnp.bfloat16)


def target_kernel(ids, *refs):
    early_ref, o_ref = refs[-2:]

    @pl.when(ids[9] == 1)
    def _():
        o_ref[...] = early_ref[...]

    @pl.when(ids[9] == 0)
    def _():
        column = 0
        for group in range(len(refs[:-2]) // 4):
            blocks = refs[4 * group : 4 * group + 4]
            piece, span = blocks[0].shape
            for slot, ref in zip((5, 7, 6, 8), blocks):
                rows = pl.ds(pl.multiple_of(ids[slot] * piece, piece), piece)
                o_ref[rows, column : column + span] = ref[...]
            column += span


def source_kernel(ids, *refs):
    moved, early_ref, o_ref = refs[:-2], refs[-2], refs[-1]
    span = moved[0].shape[1]

    @pl.when(ids[9] == 1)
    def _():
        for index, ref in enumerate(moved):
            o_ref[:, index * span : (index + 1) * span] = ref[...]

    @pl.when(ids[9] == 0)
    def _():
        o_ref[...] = early_ref[...]


def local_pairs(chunks, source_rows, target_rows, attn_weights, gains, lengths):
    n_section = lax.axis_size("section")
    n_encoder = n_section // 2
    section = lax.axis_index("section")
    here = lax.axis_index("fsdp")
    is_encoder = section < n_encoder
    from_encoder = jnp.logical_and(section >= 1, section <= n_encoder)
    ids = jnp.stack(
        [
            is_encoder.astype(jnp.int32),
            here // 2,
            here % 2,
            1 - here // 2,
            lengths[0],
            here,
            here ^ 2,
            here ^ 1,
            here ^ 3,
            from_encoder.astype(jnp.int32),
        ]
    ).astype(jnp.int32)
    own, width = source_rows.shape
    piece = own // chunks
    block = (piece, width)

    def to_sibling(value):
        return lax.ppermute(value, "fsdp", [(0, 1), (1, 0), (2, 3), (3, 2)])

    def across(value):
        return lax.ppermute(value, "fsdp", [(0, 2), (2, 0), (1, 3), (3, 1)])

    def onward(value, first, last):
        pairs = [(s, (s + 1) % n_section) for s in range(first, last)]
        return lax.ppermute(value, "section", pairs)

    normed, *pieces = norm_rows(ids, source_rows, gains, chunks)
    near = to_sibling(normed)
    remote = []
    for i in range(chunks):
        remote.append(across(pieces[i]))
    early_source = onward(source_rows, n_encoder, n_section)
    early_target = onward(target_rows, 0, n_encoder)
    qkv = qkv_rows(ids, [normed], [near], target_rows, gains, attn_weights, 1, None)
    remote_near = []
    for i in range(chunks):
        remote_near.append(to_sibling(remote[i]))
    qkv = qkv_rows(ids, remote, remote_near, target_rows, gains, attn_weights, 3, qkv)

    context = attend_rows(ids, qkv, attn_weights.shape[3])
    span = width // PARTS
    part = target_rows.shape[0] // 4
    block = (own, span)
    moved = []
    for i in range(PARTS):
        keep, send = out_chunk(ids, context, attn_weights, i, PARTS)
        taken = to_sibling(send)
        for_other = small_call(
            pair_kernel, ids,
            [keep, taken], [(block, (1, 0)), (block, (1, 0))], block,
        )
        crossed = across(for_other)
        new = small_call(
            final_kernel, ids,
            [keep, taken, crossed, source_rows, target_rows],
            [(block, (0, 0))] * 3 + [(block, (0, i)), ((part, span), ("here", i))],
            block,
        )
        moved.append(onward(new, 0, n_section))

    groups = []
    for members in (moved[:-1], moved[-1:]):
        mine = jnp.concatenate([m[:part] for m in members], axis=1)
        other = across(mine)
        sibling = to_sibling(mine)
        diagonal = to_sibling(other)
        groups += [mine, sibling, other, diagonal]
    source_next = small_call(
        source_kernel, ids,
        [*moved, early_source],
        [(block, (0, 0))] * PARTS + [((own, width), (0, 0))],
        (own, width),
    )
    target_next = small_call(
        target_kernel, ids,
        [*groups, early_target],
        [(g.shape, (0, 0)) for g in groups] + [(target_rows.shape, (0, 0))],
        target_rows.shape,
    )
    return (source_next, target_next)


def solution(mesh):
    in_specs = (
        P(("section", "fsdp"), None),
        P("section", None),
        P("section", None, None, "fsdp"),
        P("section", None),
        P("section"),
    )
    out_specs = (P(("section", "fsdp"), None), P("section", None))

    def shape_test(source_rows, target_rows, attn_weights, gains, lengths):
        n_section, n_fsdp = mesh.shape["section"], mesh.shape["fsdp"]
        own = source_rows.shape[0] // (n_section * n_fsdp)
        part = target_rows.shape[0] // (n_section * n_fsdp)
        paired = (
            n_fsdp == 4
            and part * n_section * n_fsdp == target_rows.shape[0]
            and part % 16 == 0
            and own % part == 0
            and attn_weights.shape[3] // n_fsdp % 256 == 0
            and attn_weights.shape[2] % (256 * PARTS) == 0
        )
        return own // part if paired else 0

    def mapped(body):
        return jax.shard_map(
            body, mesh=mesh, in_specs=in_specs, out_specs=out_specs, check_vma=False
        )

    def run(*arrays):
        chunks = shape_test(*arrays)
        if not chunks:
            return mapped(local_general)(*arrays)
        step = mapped(functools.partial(local_pairs, chunks))
        return step(*arrays)

    return run
```

```python
import functools
import jax
import jax.numpy as jnp
from jax import lax
from jax.experimental import pallas as pl
from jax.experimental.pallas import tpu as pltpu
from jax.sharding import PartitionSpec as P

HEAD_DIM = 64
LOG2E = 1.4426950408889634


def shifted(value, axis, steps):
    count = lax.axis_size(axis)
    pairs = [(source, (source + steps) % count) for source in range(count)]
    return lax.ppermute(value, axis, pairs)


def rms_norm(block_rows, gain_row):
    widened = block_rows.astype(jnp.float32)
    inverse_rms = lax.rsqrt(jnp.mean(widened * widened, axis=-1, keepdims=True) + 1e-06)
    return (widened * inverse_rms * gain_row).astype(jnp.bfloat16)


def project(block_rows, weight):
    return jnp.dot(block_rows, weight, preferred_element_type=jnp.float32).astype(jnp.bfloat16)


def attend(queries, key_rows, values, length):
    query_count = queries.shape[0]
    key_count = key_rows.shape[0]
    head_count = queries.shape[1] // HEAD_DIM
    query_heads = queries.reshape(query_count, head_count, HEAD_DIM)
    key_heads = key_rows.reshape(key_count, head_count, HEAD_DIM)
    value_heads = values.reshape(key_count, head_count, HEAD_DIM)
    scores = (
        jnp.einsum("qhc,khc->hqk", query_heads, key_heads, preferred_element_type=jnp.float32)
        * 0.125
    )
    key_valid = jnp.arange(key_count, dtype=jnp.int32) < length
    scores = jnp.where(key_valid[None, None, :], scores, -1000000000.0)
    row_max = jnp.max(scores, axis=-1, keepdims=True)
    expo = jnp.exp(scores - row_max)
    soft = (expo / jnp.sum(expo, axis=-1, keepdims=True)).astype(jnp.bfloat16)
    context = jnp.einsum("hqk,khc->qhc", soft, value_heads, preferred_element_type=jnp.float32)
    return context.reshape(query_count, head_count * HEAD_DIM).astype(jnp.bfloat16)


def out_partial(context, out_weight):
    return lax.dot_general(
        context, out_weight, (((1,), (1,)), ((), ())), preferred_element_type=jnp.float32
    )


def local_general(source_rows, target_rows, attn_weights, gains, lengths):
    section_index = lax.axis_index("section")
    encoder_section = section_index < lax.axis_size("section") // 2
    weights = attn_weights[0]
    gain_row = gains[0]
    length = lengths[0]
    source_whole = lax.all_gather(source_rows, "fsdp", axis=0, tiled=True)

    def encoder_work(whole_rows, target_block):
        normed = rms_norm(whole_rows, gain_row)
        context = attend(
            project(normed, weights[0]),
            project(normed, weights[1]),
            project(normed, weights[2]),
            length,
        )
        return (out_partial(context, weights[3]), jnp.zeros(target_block.shape, jnp.float32))

    def decoder_work(whole_rows, target_block):
        normed = rms_norm(target_block, gain_row)
        context = attend(
            project(normed, weights[0]),
            project(whole_rows, weights[1]),
            project(whole_rows, weights[2]),
            length,
        )
        return (jnp.zeros(whole_rows.shape, jnp.float32), out_partial(context, weights[3]))

    source_terms, target_terms = lax.cond(
        encoder_section, encoder_work, decoder_work, source_whole, target_rows
    )
    source_sum = lax.psum_scatter(
        source_terms.astype(jnp.bfloat16), "fsdp", scatter_dimension=0, tiled=True
    ).astype(jnp.float32)
    source_new = (source_rows.astype(jnp.float32) + source_sum).astype(jnp.bfloat16)
    target_sum = lax.psum(target_terms.astype(jnp.bfloat16), "fsdp").astype(jnp.float32)
    target_new = (target_rows.astype(jnp.float32) + target_sum).astype(jnp.bfloat16)
    source_next, target_next = shifted((source_new, target_new), "section", 1)
    return (source_next, target_next)


PARAMS = pltpu.CompilerParams(vmem_limit_bytes=24 * 1024 * 1024)
PARTS = 4
WEIGHT_PARAMS = pltpu.CompilerParams(vmem_limit_bytes=42 * 1024 * 1024)


def norm_kernel(ids, x_ref, gain_ref, *outs):
    piece = outs[1].shape[0]

    def put(value):
        outs[0][...] = value
        for index, out in enumerate(outs[1:]):
            out[...] = value[index * piece : (index + 1) * piece]

    @pl.when(ids[0] == 1)
    def _():
        put(rms_norm(x_ref[...], gain_ref[...]))

    @pl.when(ids[0] == 0)
    def _():
        put(x_ref[...])


def norm_rows(ids, rows, gains, chunks):
    count, width = rows.shape
    shapes = [(count, width)] + [(count // chunks, width)] * chunks
    return pl.pallas_call(
        norm_kernel,
        grid_spec=pltpu.PrefetchScalarGridSpec(
            num_scalar_prefetch=1,
            grid=(1,),
            in_specs=[
                pl.BlockSpec((count, width), lambda i, s: (0, 0)),
                pl.BlockSpec((1, width), lambda i, s: (0, 0)),
            ],
            out_specs=[pl.BlockSpec(shape, lambda i, s: (0, 0)) for shape in shapes],
        ),
        out_shape=[jax.ShapeDtypeStruct(shape, jnp.bfloat16) for shape in shapes],
        compiler_params=PARAMS,
        cost_estimate=pl.CostEstimate(
            flops=count * width * 200, bytes_accessed=count * width * 4, transcendentals=0
        ),
        name="norm_rows",
    )(ids, rows, gains)


def qkv_kernel(n_pieces, n_query, ids, *refs):
    pieces = refs[:n_pieces]
    sibling_pieces = refs[n_pieces : 2 * n_pieces]
    y_ref, gain_ref, w_ref = refs[2 * n_pieces : 2 * n_pieces + 3]
    o_ref, x_all, y_all = refs[-3:]
    step = pl.program_id(0)
    encoder, core = ids[0], ids[2]
    rows = x_all.shape[0] // 2
    piece = rows // n_pieces

    @pl.when(step == 0)
    def _():
        for index in range(n_pieces):
            mine = pl.multiple_of(core * rows + index * piece, piece)
            other = pl.multiple_of((1 - core) * rows + index * piece, piece)
            x_all[pl.ds(mine, piece), :] = pieces[index][...]
            x_all[pl.ds(other, piece), :] = sibling_pieces[index][...]

        @pl.when(encoder == 0)
        def _():
            y_all[...] = rms_norm(y_ref[...], gain_ref[...])

    from_target = jnp.logical_and(encoder == 0, step < n_query)

    @pl.when(jnp.logical_not(from_target))
    def _():
        o_ref[...] = jnp.dot(
            x_all[...], w_ref[...], preferred_element_type=jnp.float32
        ).astype(jnp.bfloat16)

    @pl.when(from_target)
    def _():
        queries = jnp.dot(
            y_all[...], w_ref[...], preferred_element_type=jnp.float32
        ).astype(jnp.bfloat16)
        half = queries.shape[0] // 2
        o_ref[...] = jnp.zeros_like(o_ref)
        o_ref[0:half, :] = queries[:half]
        o_ref[rows : rows + half, :] = queries[half:]


def qkv_rows(ids, pieces, sibling_pieces, target_rows, gains, attn_weights, slot_index, into):
    n_pieces = len(pieces)
    rows = sum(p.shape[0] for p in pieces)
    width = pieces[0].shape[1]
    inner = attn_weights.shape[3]
    tile = 256
    per = inner // tile
    part = target_rows.shape[0] // 2
    in_specs = [pl.BlockSpec(p.shape, lambda i, s: (0, 0)) for p in pieces + sibling_pieces]
    in_specs += [
        pl.BlockSpec((part, width), lambda i, s: (s[slot_index], 0)),
        pl.BlockSpec((1, width), lambda i, s: (0, 0)),
        pl.BlockSpec((None, None, width, tile), lambda i, s: (0, i // per, 0, i % per)),
    ]
    operands = [ids, *pieces, *sibling_pieces, target_rows, gains, attn_weights]
    aliases = {}
    if into is not None:
        in_specs.append(pl.BlockSpec(memory_space=pl.ANY))
        aliases = {len(operands): 0}
        operands.append(into)
    return pl.pallas_call(
        functools.partial(qkv_kernel, n_pieces, per),
        grid_spec=pltpu.PrefetchScalarGridSpec(
            num_scalar_prefetch=1,
            grid=(3 * per,),
            in_specs=in_specs,
            out_specs=pl.BlockSpec((2 * rows, tile), lambda i, s: (s[slot_index], i)),
            scratch_shapes=[
                pltpu.VMEM((2 * rows, width), jnp.bfloat16),
                pltpu.VMEM((part, width), jnp.bfloat16),
            ],
        ),
        out_shape=jax.ShapeDtypeStruct((4 * rows, 3 * inner), jnp.bfloat16),
        input_output_aliases=aliases,
        cost_estimate=pl.CostEstimate(
            flops=2 * 2 * rows * width * 3 * inner,
            bytes_accessed=2 * width * 3 * inner,
            transcendentals=0,
        ),
        compiler_params=WEIGHT_PARAMS,
        name="qkv_rows",
    )(*operands)


def attend_kernel(ids, q_ref, k_ref, v_ref, ctx):
    length = ids[4]
    rows, inner = q_ref.shape
    count = k_ref.shape[0]
    valid = lax.broadcasted_iota(jnp.int32, (rows, count), 1) < length
    low = lax.broadcasted_iota(jnp.int32, (rows, 2 * HEAD_DIM), 1) < HEAD_DIM
    for pair in range(inner // (2 * HEAD_DIM)):
        lanes = slice(pair * 2 * HEAD_DIM, (pair + 1) * 2 * HEAD_DIM)
        q_pair = q_ref[:, lanes]
        k_pair = k_ref[:, lanes]
        v_pair = v_ref[:, lanes]
        parts = []
        for head in range(2):
            mask = low if head == 0 else jnp.logical_not(low)
            q_head = jnp.where(mask, q_pair, jnp.zeros_like(q_pair))
            scores = lax.dot_general(
                q_head, k_pair, (((1,), (1,)), ((), ())), preferred_element_type=jnp.float32
            )
            scores = jnp.where(valid, scores, -8000000000.0)
            row_max = jnp.max(scores, axis=-1, keepdims=True)
            expo = jnp.exp2((scores - row_max) * (0.125 * LOG2E))
            total = jnp.sum(expo, axis=-1, keepdims=True)
            soft = (expo * (1.0 / total)).astype(jnp.bfloat16)
            parts.append(jnp.dot(soft, v_pair, preferred_element_type=jnp.float32))
        ctx[:, lanes] = jnp.where(low, parts[0], parts[1]).astype(jnp.bfloat16)


def attend_rows(ids, qkv, inner):
    total = qkv.shape[0]
    return pl.pallas_call(
        attend_kernel,
        grid_spec=pltpu.PrefetchScalarGridSpec(
            num_scalar_prefetch=1,
            grid=(1,),
            in_specs=[
                pl.BlockSpec((total, inner), lambda i, s: (0, 0)),
                pl.BlockSpec((total, inner), lambda i, s: (0, 1)),
                pl.BlockSpec((total, inner), lambda i, s: (0, 2)),
            ],
            out_specs=pl.BlockSpec((total, inner), lambda i, s: (0, 0)),
        ),
        out_shape=jax.ShapeDtypeStruct((total, inner), jnp.bfloat16),
        compiler_params=PARAMS,
        cost_estimate=pl.CostEstimate(
            flops=40 * total * total * inner, bytes_accessed=8 * total * inner, transcendentals=0
        ),
        name="attend_rows",
    )(ids, qkv, qkv, qkv)


def out_kernel(ids, c0, c1, c2, c3, w_ref, source_ref, target_ref, base_ref, keep_ref, send_ref):
    context = jnp.concatenate([c[...] for c in (c0, c1, c2, c3)], axis=0)
    terms = out_partial(context, w_ref[...]).astype(jnp.bfloat16)
    half = terms.shape[0] // 2
    own = half // 2
    mine = terms[:own].astype(jnp.float32)
    base_ref[...] = source_ref[...].astype(jnp.float32) + mine
    keep_ref[...] = terms[own:half]
    send_ref[...] = terms[half:]

    @pl.when(ids[0] == 0)
    def _():
        part = target_ref.shape[0]
        base_ref[0:part, :] = target_ref[...].astype(jnp.float32) + mine[:part]


def out_chunk(ids, context, attn_weights, source_rows, target_rows, chunk, parts):
    total, inner = context.shape
    span = attn_weights.shape[2] // parts
    tile = span // 2

    def rows_spec(slot):
        return pl.BlockSpec((total // 4, inner), lambda i, s: (s[slot], 0))

    half = jax.ShapeDtypeStruct((total // 2, span), jnp.bfloat16)
    return pl.pallas_call(
        out_kernel,
        grid_spec=pltpu.PrefetchScalarGridSpec(
            num_scalar_prefetch=1,
            grid=(2,),
            in_specs=[
                rows_spec(5),
                rows_spec(6),
                rows_spec(7),
                rows_spec(8),
                pl.BlockSpec((None, None, tile, inner), lambda i, s: (0, 3, 2 * chunk + i, 0)),
                pl.BlockSpec((total // 4, tile), lambda i, s: (0, 2 * chunk + i)),
                pl.BlockSpec((target_rows.shape[0] // 4, tile), lambda i, s: (s[5], 2 * chunk + i)),
            ],
            out_specs=[
                pl.BlockSpec((total // 4, tile), lambda i, s: (0, i)),
                pl.BlockSpec((total // 4, tile), lambda i, s: (0, i)),
                pl.BlockSpec((total // 2, tile), lambda i, s: (0, i)),
            ],
        ),
        out_shape=[
            jax.ShapeDtypeStruct((total // 4, span), jnp.float32),
            jax.ShapeDtypeStruct((total // 4, span), jnp.bfloat16),
            half,
        ],
        compiler_params=WEIGHT_PARAMS,
        cost_estimate=pl.CostEstimate(
            flops=2 * total * span * inner, bytes_accessed=2 * span * inner, transcendentals=0
        ),
        name="out_chunk",
    )(ids, context, context, context, context, attn_weights, source_rows, target_rows)


def small_call(kernel, ids, operands, blocks, out_shape):
    def spec(shape, index):
        return pl.BlockSpec(shape, lambda i, s: index)

    return pl.pallas_call(
        kernel,
        grid_spec=pltpu.PrefetchScalarGridSpec(
            num_scalar_prefetch=1,
            grid=(1,),
            in_specs=[spec(*b) for b in blocks],
            out_specs=pl.BlockSpec(out_shape, lambda i, s: (0, 0)),
        ),
        out_shape=jax.ShapeDtypeStruct(out_shape, jnp.bfloat16),
        compiler_params=PARAMS,
        cost_estimate=pl.CostEstimate(
            flops=out_shape[0] * out_shape[1] * 200,
            bytes_accessed=out_shape[0] * out_shape[1] * 8,
            transcendentals=0,
        ),
    )(ids, *operands)


def pair_kernel(ids, keep_ref, taken_ref, o_ref):
    o_ref[...] = (
        keep_ref[...].astype(jnp.float32) + taken_ref[...].astype(jnp.float32)
    ).astype(jnp.bfloat16)


def final_kernel(ids, base_ref, taken_ref, crossed_ref, o_ref):
    f32 = jnp.float32
    total = base_ref[...] + taken_ref[...].astype(f32) + crossed_ref[...].astype(f32)
    o_ref[...] = total.astype(jnp.bfloat16)


def target_kernel(ids, *refs):
    early_ref, o_ref = refs[-2:]

    @pl.when(ids[9] == 1)
    def _():
        o_ref[...] = early_ref[...]

    @pl.when(ids[9] == 0)
    def _():
        column = 0
        for group in range(len(refs[:-2]) // 4):
            blocks = refs[4 * group : 4 * group + 4]
            piece, span = blocks[0].shape
            for slot, ref in zip((5, 7, 6, 8), blocks):
                rows = pl.ds(pl.multiple_of(ids[slot] * piece, piece), piece)
                o_ref[rows, column : column + span] = ref[...]
            column += span


def source_kernel(ids, *refs):
    moved, early_ref, o_ref = refs[:-2], refs[-2], refs[-1]
    span = moved[0].shape[1]

    @pl.when(ids[9] == 1)
    def _():
        for index, ref in enumerate(moved):
            o_ref[:, index * span : (index + 1) * span] = ref[...]

    @pl.when(ids[9] == 0)
    def _():
        o_ref[...] = early_ref[...]


def local_pairs(chunks, source_rows, target_rows, attn_weights, gains, lengths):
    n_section = lax.axis_size("section")
    n_encoder = n_section // 2
    section = lax.axis_index("section")
    here = lax.axis_index("fsdp")
    is_encoder = section < n_encoder
    from_encoder = jnp.logical_and(section >= 1, section <= n_encoder)
    ids = jnp.stack(
        [
            is_encoder.astype(jnp.int32),
            here // 2,
            here % 2,
            1 - here // 2,
            lengths[0],
            here,
            here ^ 2,
            here ^ 1,
            here ^ 3,
            from_encoder.astype(jnp.int32),
        ]
    ).astype(jnp.int32)
    own, width = source_rows.shape
    piece = own // chunks
    block = (piece, width)

    def to_sibling(value):
        return lax.ppermute(value, "fsdp", [(0, 1), (1, 0), (2, 3), (3, 2)])

    def across(value):
        return lax.ppermute(value, "fsdp", [(0, 2), (2, 0), (1, 3), (3, 1)])

    def onward(value, first, last):
        pairs = [(s, (s + 1) % n_section) for s in range(first, last)]
        return lax.ppermute(value, "section", pairs)

    normed, *pieces = norm_rows(ids, source_rows, gains, chunks)
    near = to_sibling(normed)
    remote = []
    for i in range(chunks):
        remote.append(across(pieces[i]))
    early_source = onward(source_rows, n_encoder, n_section)
    early_target = onward(target_rows, 0, n_encoder)
    qkv = qkv_rows(ids, [normed], [near], target_rows, gains, attn_weights, 1, None)
    remote_near = []
    for i in range(chunks):
        remote_near.append(to_sibling(remote[i]))
    qkv = qkv_rows(ids, remote, remote_near, target_rows, gains, attn_weights, 3, qkv)

    context = attend_rows(ids, qkv, attn_weights.shape[3])
    span = width // PARTS
    part = target_rows.shape[0] // 4
    block = (own, span)
    moved = []
    for i in range(PARTS):
        base, keep, send = out_chunk(ids, context, attn_weights, source_rows, target_rows, i, PARTS)
        taken = to_sibling(send)
        for_other = small_call(
            pair_kernel, ids,
            [keep, taken], [(block, (0, 0)), (block, (1, 0))], block,
        )
        crossed = across(for_other)
        new = small_call(
            final_kernel, ids,
            [base, taken, crossed], [(block, (0, 0))] * 3, block,
        )
        moved.append(onward(new, 0, n_section))

    groups = []
    for members in (moved[:-1], moved[-1:]):
        mine = jnp.concatenate([m[:part] for m in members], axis=1)
        other = across(mine)
        sibling = to_sibling(mine)
        diagonal = to_sibling(other)
        groups += [mine, sibling, other, diagonal]
    source_next = small_call(
        source_kernel, ids,
        [*moved, early_source],
        [(block, (0, 0))] * PARTS + [((own, width), (0, 0))],
        (own, width),
    )
    target_next = small_call(
        target_kernel, ids,
        [*groups, early_target],
        [(g.shape, (0, 0)) for g in groups] + [(target_rows.shape, (0, 0))],
        target_rows.shape,
    )
    return (source_next, target_next)


def solution(mesh):
    in_specs = (
        P(("section", "fsdp"), None),
        P("section", None),
        P("section", None, None, "fsdp"),
        P("section", None),
        P("section"),
    )
    out_specs = (P(("section", "fsdp"), None), P("section", None))

    def shape_test(source_rows, target_rows, attn_weights, gains, lengths):
        n_section, n_fsdp = mesh.shape["section"], mesh.shape["fsdp"]
        own = source_rows.shape[0] // (n_section * n_fsdp)
        part = target_rows.shape[0] // (n_section * n_fsdp)
        paired = (
            n_fsdp == 4
            and part * n_section * n_fsdp == target_rows.shape[0]
            and part % 16 == 0
            and own % part == 0
            and attn_weights.shape[3] // n_fsdp % 256 == 0
            and attn_weights.shape[2] % (256 * PARTS) == 0
        )
        return own // part if paired else 0

    def mapped(body):
        return jax.shard_map(
            body, mesh=mesh, in_specs=in_specs, out_specs=out_specs, check_vma=False
        )

    def run(*arrays):
        chunks = shape_test(*arrays)
        if not chunks:
            return mapped(local_general)(*arrays)
        step = mapped(functools.partial(local_pairs, chunks))
        return step(*arrays)

    return run
```
